32 devices in a mesh: seq: 8 (over z, y), head: 4 (over x, core).
Axes of the slice: x: 2, y: 2, z: 4, core: 2. Of those that a mesh axis runs over, the one named last changes fastest.
Arguments:
- layer_in: bfloat16 [4096, 2048], P('seq', 'head'), may hold values from -6 to 6
- query_weight: bfloat16 [2048, 1024], P(None, 'head'), may hold values from -0.125 to 0.125
- key_weight: bfloat16 [2048, 1024], P(None, 'head'), may hold values from -0.125 to 0.125
- value_weight: bfloat16 [2048, 1024], P(None, 'head'), may hold values from -0.125 to 0.125
- gate_weight: bfloat16 [2048, 1024], P(None, 'head'), may hold values from -0.125 to 0.125
- beta_weight: bfloat16 [2048, 8], P(None, 'head'), may hold values from -0.125 to 0.125
- decay_weight: bfloat16 [2048, 8], P(None, 'head'), may hold values from -0.125 to 0.125
- conv_weight: float32 [4, 3, 1024], P(None, None, 'head'), may hold values from -3 to 3
- decay_log: float32 [8], P('head'), as said below
- beta_bias: float32 [8], P('head'), as said below
- decay_bias: float32 [8], P('head'), may hold values from -1 to 1
- norm_gain: float32 [128], replicated, may hold values from 0.1 to 1.9
- out_weight: bfloat16 [1024, 2048], P('head'), may hold values from -0.1875 to 0.1875
Outputs:
- layer_out: bfloat16 [4096, 2048], P('seq', 'head')
The draws below stay inside these ranges and needn't reach their ends.
Inputs may be any that keep to these rules, and one draw needn't show every extreme that they name: decay_log lies between log(0.1 / 4096) and log(0.05). beta_bias lies between log(0.5 * 128 / 4096) and 1.
All inputs are finite; a program needn't handle non-finite values.
Results may differ from the reference program's by a relative error of at most 0.0049.
Values may be sent and summed in bfloat16 or wider, within the bound.
No kernel may reach another device: no remote copies, remote signals or barrier semaphores. Data moves between devices by JAX's collectives and lax.ppermute only.
A program may use at most 128 MiB of HBM per device.

```python
import jax
import jax.numpy as jnp
from jax import lax

D = 2048
HEADS = 8
HDIM = 128
CONV = 4
BLOCK = 128
TOKENS = 4096


def head_kinds(key):
    pair_count = HEADS // 2
    pick_one = jax.random.randint(jax.random.fold_in(key, 31), (pair_count,), 0, 2)
    rolled = jax.random.randint(jax.random.fold_in(key, 32), (pair_count,), 0, 100)
    limit = 25
    both_slow = rolled < limit
    first_slow = (pick_one == 0) | both_slow
    second_slow = (pick_one == 1) | both_slow
    return jnp.stack([first_slow, second_slow], axis=1).reshape(HEADS)


def draw_decay_log(key, part):
    slow_heads = head_kinds(key)
    spread = jax.random.uniform(jax.random.fold_in(key, 41), (HEADS,), jnp.float32)
    slow_rate = jnp.log((0.1 + 0.4 * spread) / TOKENS)
    fast_rate = jnp.log(0.02 + 0.03 * spread)
    return jnp.where(slow_heads, slow_rate, fast_rate).astype(jnp.float32)


def draw_beta_bias(key, part):
    slow_heads = head_kinds(key)
    spread = jax.random.uniform(jax.random.fold_in(key, 42), (HEADS,), jnp.float32)
    slow_bias = jnp.log((0.5 + 0.5 * spread) * HDIM / TOKENS)
    fast_bias = 2.0 * spread - 1.0
    return jnp.where(slow_heads, slow_bias, fast_bias).astype(jnp.float32)


def shard_levels(rng, shape, shards, smallest, high):
    loudness = 1.0
    for position, shards_of in shards:
        steps = jax.random.uniform(jax.random.fold_in(jax.random.fold_in(rng, 6), position), (shards_of,), jnp.float32, smallest / len(shards), high / len(shards))
        loudness = loudness * jnp.repeat(jnp.exp(steps), shape[position] // shards_of).reshape((-1,) + (1,) * (len(shape) - 1 - position))
    return loudness


def bell_draw(rng, extent, width, reach, pieces=(), kind=jnp.bfloat16):
    values = width * jax.random.normal(rng, extent, jnp.float32)
    if pieces:
        values = values * shard_levels(rng, extent, pieces, -0.22, 0.18)
    return jnp.clip(values, -reach, reach).astype(kind)


def setup_inputs(seed: int = 0) -> dict:
    seeds = jax.random.split(jax.random.key(seed), 14)
    layer_in = bell_draw(seeds[0], (TOKENS, D), 1.0, 6.0, ((0, 8), (1, 4)))
    query_weight = bell_draw(seeds[1], (D, HEADS * HDIM), D ** -0.5, 0.125, ((1, 4),))
    key_weight = bell_draw(seeds[2], (D, HEADS * HDIM), D ** -0.5, 0.125, ((1, 4),))
    value_weight = bell_draw(seeds[3], (D, HEADS * HDIM), D ** -0.5, 0.125, ((1, 4),))
    gate_weight = bell_draw(seeds[4], (D, HEADS * HDIM), D ** -0.5, 0.125, ((1, 4),))
    beta_weight = bell_draw(seeds[5], (D, HEADS), D ** -0.5, 0.125, ((1, 4),))
    decay_weight = bell_draw(seeds[6], (D, HEADS), D ** -0.5, 0.125, ((1, 4),))
    conv_weight = bell_draw(seeds[7], (CONV, 3, HEADS * HDIM), 0.5, 3.0, ((2, 4),), jnp.float32)
    decay_log = draw_decay_log(jax.random.fold_in(seeds[13], 71), 0)
    beta_bias = draw_beta_bias(jax.random.fold_in(seeds[13], 71), 0)
    decay_bias = jnp.clip(jax.random.uniform(seeds[10], (HEADS,), jnp.float32, -1.0, 1.0) * shard_levels(seeds[10], (HEADS,), ((0, 4),), -0.4, 0.0), -1.0, 1.0)
    norm_gain = jnp.clip(1.0 + 0.18 * jax.random.normal(seeds[11], (HDIM,), jnp.float32), 0.1, 1.9)
    out_weight = bell_draw(seeds[12], (HEADS * HDIM, D), (HEADS * HDIM) ** -0.5, 0.1875, ((0, 4),))
    return {"layer_in": layer_in, "query_weight": query_weight, "key_weight": key_weight, "value_weight": value_weight, "gate_weight": gate_weight, "beta_weight": beta_weight, "decay_weight": decay_weight, "conv_weight": conv_weight, "decay_log": decay_log, "beta_bias": beta_bias, "decay_bias": decay_bias, "norm_gain": norm_gain, "out_weight": out_weight}


exact_mode = lax.Precision.HIGHEST
norm_floor = 0.0001

def causal_conv(values, kernel):
    taps = kernel.shape[0]
    summed = kernel[0] * values
    for offset in range(1, taps):
        shifted = jnp.concatenate([jnp.zeros((offset, values.shape[1]), jnp.float32), values[:-offset]], axis=0)
        summed = summed + kernel[offset] * shifted
    return jax.nn.silu(summed)

def unit_rows(values):
    return values * lax.rsqrt(lax.optimization_barrier(jnp.sum(values * values, axis=-1, keepdims=True)) + 1.0)

def block_terms(queries, key_rows, values, beta_gate, log_decay):
    length = log_decay.shape[-1]
    running = jnp.cumsum(log_decay, axis=-1)
    row_index = lax.broadcasted_iota(jnp.int32, (length, length), 0)
    col_index = lax.broadcasted_iota(jnp.int32, (length, length), 1)
    within = row_index >= col_index
    before = row_index > col_index
    spread = running[..., :, None] - running[..., None, :]
    decay_matrix = jnp.where(within, jnp.exp(jnp.minimum(spread, 0.0)), 0.0)
    key_gram = jnp.einsum('...rd,...sd->...rs', key_rows, key_rows, precision=exact_mode)
    lower_part = jnp.where(before, beta_gate[..., :, None] * decay_matrix * key_gram, 0.0)
    system = lower_part + jnp.eye(length, dtype=jnp.float32)
    growth = jnp.exp(running)
    right_side = jnp.concatenate([beta_gate[..., None] * values, (beta_gate * growth)[..., None] * key_rows], axis=-1)
    solved = lax.linalg.triangular_solve(system, right_side, left_side=True, lower=True, unit_diagonal=True)
    value_dim = values.shape[-1]
    fixed_rows = solved[..., :value_dim]
    erased = solved[..., value_dim:]
    query_key = jnp.einsum('...rd,...sd->...rs', queries, key_rows, precision=exact_mode)
    mixing = jnp.where(within, decay_matrix * query_key, 0.0)
    local_out = jnp.einsum('...rs,...se->...re', mixing, fixed_rows, precision=exact_mode)
    reader = growth[..., None] * queries - jnp.einsum('...rs,...sd->...rd', mixing, erased, precision=exact_mode)
    tail_decay = jnp.exp(running[..., -1:] - running)
    weighted = tail_decay[..., None] * key_rows
    key_dim = key_rows.shape[-1]
    transit = jnp.exp(running[..., -1])[..., None, None] * jnp.eye(key_dim, dtype=jnp.float32) - jnp.einsum('...bd,...be->...de', weighted, erased, precision=exact_mode)
    carried = jnp.einsum('...bd,...be->...de', weighted, fixed_rows, precision=exact_mode)
    return (local_out, reader, transit, carried)

def reference(layer_in, query_weight, key_weight, value_weight, gate_weight, beta_weight, decay_weight, conv_weight, decay_log, beta_bias, decay_bias, norm_gain, out_weight):
    tokens = layer_in.shape[0]

    def project(weight):
        return jnp.dot(layer_in.astype(jnp.float32), weight.astype(jnp.float32), preferred_element_type=jnp.float32)
    mixed_query = causal_conv(project(query_weight), conv_weight[:, 0])
    mixed_key = causal_conv(project(key_weight), conv_weight[:, 1])
    mixed_value = causal_conv(project(value_weight), conv_weight[:, 2])
    queries = unit_rows(mixed_query.reshape(tokens, HEADS, HDIM))
    key_rows = unit_rows(mixed_key.reshape(tokens, HEADS, HDIM))
    values = mixed_value.reshape(tokens, HEADS, HDIM)
    beta_gate = jax.nn.sigmoid(project(beta_weight) + beta_bias)
    log_decay = -jnp.exp(decay_log) * jax.nn.softplus(project(decay_weight) + decay_bias)
    blocks = tokens // BLOCK

    def arrange(array):
        return array.reshape(blocks, BLOCK, HEADS, HDIM).transpose(0, 2, 1, 3)

    def arrange_gate(array):
        return array.reshape(blocks, BLOCK, HEADS).transpose(0, 2, 1)

    def advance(carry_state, inputs):
        local_out, reader, transit, carried = block_terms(*inputs)
        output = local_out + jnp.einsum('hrd,hde->hre', reader, carry_state, precision=exact_mode)
        carry_state = jnp.einsum('hde,hef->hdf', transit, carry_state, precision=exact_mode) + carried
        return (carry_state, output)
    zero_state = jnp.zeros((HEADS, HDIM, HDIM), jnp.float32)
    last_state, outputs = lax.scan(advance, zero_state, (arrange(queries), arrange(key_rows), arrange(values), arrange_gate(beta_gate), arrange_gate(log_decay)))
    head_out = outputs.transpose(0, 2, 1, 3).reshape(tokens, HEADS, HDIM)
    gate_rows = project(gate_weight).reshape(tokens, HEADS, HDIM)
    scaled = head_out * lax.rsqrt(lax.optimization_barrier(jnp.mean(head_out * head_out, axis=-1, keepdims=True)) + norm_floor)
    hidden = (scaled * norm_gain * jax.nn.silu(gate_rows)).reshape(tokens, HEADS * HDIM).astype(jnp.bfloat16)
    return jnp.dot(hidden.astype(jnp.float32), out_weight.astype(jnp.float32), preferred_element_type=jnp.float32).astype(jnp.bfloat16)
```

```python
import functools

import jax
import jax.numpy as jnp
from jax import lax
from jax.experimental import pallas as pl
from jax.experimental.pallas import tpu as pltpu
from jax.sharding import PartitionSpec as P

BLOCK = 128
HALO = 8
norm_floor = 0.0001
f32 = jnp.float32
bf16 = jnp.bfloat16


def split(a):
    hi = a.astype(bf16)
    return hi, (a - hi.astype(f32)).astype(bf16)


def dot(a, b):
    return lax.dot_general(a, b, (((1,), (0,)), ((), ())), preferred_element_type=f32)


def dot_nt(a, b):
    return lax.dot_general(a, b, (((1,), (1,)), ((), ())), preferred_element_type=f32)


def mm_square(a, b):
    n = b[0].shape[1]
    right = jnp.concatenate([b[0], b[1]], axis=1)
    out = dot(jnp.concatenate([a[0], a[1]], axis=1), jnp.concatenate([right, right], axis=0))
    return out[:, :n] + out[:, n:]


def mm_wide(a, b):
    left = jnp.concatenate([a[0], a[1]], axis=1)
    return dot(left, jnp.concatenate([b[0], b[0]], axis=0)) + dot(a[0], b[1])


def mm_nt(a, b):
    left = jnp.concatenate([a[0], a[1]], axis=1)
    return dot_nt(left, jnp.concatenate([b[0], b[0]], axis=1)) + dot_nt(a[0], b[1])


def iotas(n):
    return (
        lax.broadcasted_iota(jnp.int32, (n, n), 0),
        lax.broadcasted_iota(jnp.int32, (n, n), 1),
    )


def project(pieces, weight_ref, index, rows, features):
    total = None
    for mask, piece in enumerate(pieces):
        start = pl.multiple_of((index ^ mask) * features, features)
        part = dot(piece(rows), weight_ref[pl.ds(start, features), :])
        total = part if total is None else total + part
    return total


def conv_rows(ext_ref, conv_ref, channel, taps, tokens):
    summed = None
    for s in range(taps):
        part = conv_ref[pl.ds(s * 3 + channel, 1), :] * ext_ref[pl.ds(HALO - s, tokens), :]
        summed = part if summed is None else summed + part
    return jax.nn.silu(summed)


def unit_heads(values, heads, dim):
    parts = []
    for h in range(heads):
        v = values[:, h * dim : (h + 1) * dim]
        parts.append(v * lax.rsqrt(jnp.sum(v * v, axis=-1, keepdims=True) + 1.0))
    return jnp.concatenate(parts, axis=1)


def decay_of(running, running_t, lane):
    row, col = iotas(BLOCK)
    spread = running[:, lane : lane + 1] - running_t[lane : lane + 1, :]
    return jnp.where(row >= col, jnp.exp(jnp.minimum(spread, 0.0)), 0.0)


def key_kernel(masks, chunks, heads, dim, taps, *refs):
    index = refs[0][0]
    x_refs = refs[1 : 1 + masks * chunks]
    refs = refs[1 + masks * chunks :]
    halo_refs = refs[:masks]
    key_w, value_w, gate_w, conv_ref, bias_ref, rate_ref = refs[masks : masks + 6]
    k_out, run_out, solved_out, prefix_out, slab_out, slab_low_out, ext = refs[masks + 6 :]
    tokens = k_out.shape[0]
    features = x_refs[0].shape[1]
    step = tokens // chunks
    pieces = [
        (lambda c, m=m: x_refs[m * chunks + c][...]) for m in range(masks)
    ]
    halos = [(lambda c, m=m: halo_refs[m][...]) for m in range(masks)]

    def mixed(weight, channel):
        ext[pl.ds(0, HALO), :] = project(halos, weight, index, 0, features)
        for c in range(chunks):
            ext[pl.ds(HALO + c * step, step), :] = project(pieces, weight, index, c, features)
        return conv_rows(ext, conv_ref, channel, taps, tokens)

    gates = jnp.concatenate(
        [project(pieces, gate_w, index, c, features) for c in range(chunks)], axis=0
    )
    z = gates + bias_ref[...]
    beta = jax.nn.sigmoid(z)
    log_decay = -rate_ref[...] * (jnp.maximum(z, 0.0) + jnp.log(1.0 + jnp.exp(-jnp.abs(z))))
    keys = unit_heads(mixed(key_w, 1), heads, dim)
    k_out[...] = keys
    values = mixed(value_w, 2)
    blocks = tokens // BLOCK
    row, col = iotas(BLOCK)
    triangle = jnp.where(row >= col, 1.0, 0.0).astype(f32)
    eye = jnp.where(row == col, 1.0, 0.0).astype(f32)
    units = [(b, h) for b in range(blocks) for h in range(heads)]
    running = []
    for b in range(blocks):
        r = lax.dot_general(
            triangle,
            log_decay[b * BLOCK : (b + 1) * BLOCK],
            (((1,), (0,)), ((), ())),
            preferred_element_type=f32,
            precision=lax.Precision.HIGHEST,
        )
        run_out[pl.ds(b * BLOCK, BLOCK), :] = r
        running.append(r)
    running_t = [jnp.transpose(r) for r in running]
    k_of = {}
    lower = {}
    inverse = {}
    for b, h in units:
        k = keys[b * BLOCK : (b + 1) * BLOCK, h * dim : (h + 1) * dim]
        k_of[b, h] = k
        pair = split(k)
        bcol = beta[b * BLOCK : (b + 1) * BLOCK, h : h + 1]
        gram = mm_nt(pair, pair)
        system = jnp.where(
            row > col, bcol * decay_of(running[b], running_t[b], heads + h) * gram, 0.0
        )
        lower[b, h] = system
        link = (row // 2 == col // 2) & (row > col)
        inverse[b, h] = eye - jnp.where(link, system, 0.0)
    width = 2
    while width < BLOCK:
        link = (row // (2 * width) == col // (2 * width)) & (row // width > col // width)
        middle = {}
        pairs = {}
        for u in units:
            pairs[u] = split(inverse[u])
            middle[u] = mm_square(split(jnp.where(link, lower[u], 0.0)), pairs[u])
        for u in units:
            inverse[u] = inverse[u] - mm_square(pairs[u], split(middle[u]))
        width *= 2
    maps = {}
    solved_pair = {}
    for b, h in units:
        k = k_of[b, h]
        bcol = beta[b * BLOCK : (b + 1) * BLOCK, h : h + 1]
        rcol = running[b][:, heads + h : heads + h + 1]
        v = values[b * BLOCK : (b + 1) * BLOCK, h * dim : (h + 1) * dim]
        right = jnp.concatenate([(bcol * jnp.exp(rcol)) * k, bcol * v], axis=1)
        solved = mm_wide(split(inverse[b, h]), split(right))
        solved_out[b * heads + h] = solved
        solved_pair[b, h] = split(solved)
    for b, h in units:
        rcol = running[b][:, heads + h : heads + h + 1]
        last = rcol[BLOCK - 1 : BLOCK, :]
        weighted = jnp.transpose(jnp.exp(last - rcol) * k_of[b, h])
        moved = mm_wide(split(weighted), solved_pair[b, h])
        transit = jnp.exp(last) * eye - moved[:, :dim]
        maps[b, h] = jnp.concatenate([transit, moved[:, dim:]], axis=1)

    def compose(later, earlier):
        out = mm_wide(split(later[:, :dim]), split(earlier))
        return jnp.concatenate([out[:, :dim], out[:, dim:] + later[:, dim:]], axis=1)

    for h in range(heads):
        prefix = {1: maps[0, h]}
        spans = {(b, 1): maps[b, h] for b in range(blocks)}

        def span(start, count):
            if (start, count) not in spans:
                half = 1
                while half * 2 < count:
                    half *= 2
                spans[start, count] = compose(
                    span(start + half, count - half), span(start, half)
                )
            return spans[start, count]

        for b in range(1, blocks):
            prefix_out[h * (blocks - 1) + b - 1] = span(0, b)
        slab = span(0, blocks)
        slab_out[h] = slab
        slab_low_out[h] = slab.astype(bf16)


def query_kernel(masks, chunks, heads, dim, taps, *refs):
    index = refs[0][0]
    x_refs = refs[1 : 1 + masks * chunks]
    refs = refs[1 + masks * chunks :]
    halo_refs = refs[:masks]
    query_w, gate_w, conv_ref, gain_ref = refs[masks : masks + 4]
    q_out, gate_out, ext = refs[masks + 4 :]
    tokens = q_out.shape[0]
    features = x_refs[0].shape[1]
    step = tokens // chunks
    pieces = [(lambda c, m=m: x_refs[m * chunks + c][...]) for m in range(masks)]
    halos = [(lambda c, m=m: halo_refs[m][...]) for m in range(masks)]
    ext[pl.ds(0, HALO), :] = project(halos, query_w, index, 0, features)
    for c in range(chunks):
        ext[pl.ds(HALO + c * step, step), :] = project(pieces, query_w, index, c, features)
        gate_out[pl.ds(c * step, step), :] = (
            jax.nn.silu(project(pieces, gate_w, index, c, features)) * gain_ref[...]
        )
    q_out[...] = unit_heads(conv_rows(ext, conv_ref, 0, taps, tokens), heads, dim)


def read_kernel(heads, dim, q_ref, k_ref, run_ref, solved_ref, prefix_ref, a_out, r_out):
    tokens = q_ref.shape[0]
    blocks = tokens // BLOCK
    units = [(b, h) for b in range(blocks) for h in range(heads)]
    running = [run_ref[pl.ds(b * BLOCK, BLOCK), :] for b in range(blocks)]
    running_t = [jnp.transpose(r) for r in running]
    mixing = {}
    for b, h in units:
        q = split(q_ref[pl.ds(b * BLOCK, BLOCK), pl.ds(h * dim, dim)])
        k = split(k_ref[pl.ds(b * BLOCK, BLOCK), pl.ds(h * dim, dim)])
        mixing[b, h] = decay_of(running[b], running_t[b], heads + h) * mm_nt(q, k)
    for b, h in units:
        rows, cols = pl.ds(b * BLOCK, BLOCK), pl.ds(h * dim, dim)
        out = mm_wide(split(mixing[b, h]), split(solved_ref[b * heads + h]))
        growth = jnp.exp(running[b][:, heads + h : heads + h + 1])
        reader = growth * q_ref[rows, cols] - out[:, :dim]
        local = out[:, dim:]
        if b > 0:
            moved = mm_wide(split(reader), split(prefix_ref[h * (blocks - 1) + b - 1]))
            reader = moved[:, :dim]
            local = local + moved[:, dim:]
        a_out[rows, cols] = local
        r_out[rows, cols] = reader


def step_kernel(heads, dim, first, distance, pos_ref, got_ref, *refs):
    if first:
        own_ref, before_out, own_out, low_out = refs
    else:
        before_ref, own_ref, before_out, own_out, low_out = refs
    valid = pos_ref[0] >= distance
    row = lax.broadcasted_iota(jnp.int32, (dim, 2 * dim), 0)
    col = lax.broadcasted_iota(jnp.int32, (dim, 2 * dim), 1)
    unchanged = jnp.where(row == col, 1.0, 0.0).astype(f32)
    for h in range(heads):
        got = jnp.where(valid, got_ref[h].astype(f32), unchanged)
        low = got.astype(bf16)
        low = jnp.concatenate([low, low], axis=0)

        def after(later):
            hi, lo = split(later[:, :dim])
            out = dot(jnp.concatenate([hi, lo], axis=1), low)
            return jnp.concatenate([out[:, :dim], out[:, dim:] + later[:, dim:]], axis=1)

        own = after(own_ref[h])
        own_out[h] = own
        low_out[h] = own.astype(bf16)
        before_out[h] = got if first else after(before_ref[h])


def hidden_kernel(heads, dim, a_ref, r_ref, gate_ref, before_ref, got_ref, out_ref):
    for h in range(heads):
        cols = pl.ds(h * dim, dim)
        before = before_ref[h]
        got = got_ref[h]
        hi, lo = split(before[:, :dim])
        state = before[:, dim:] + dot(
            jnp.concatenate([hi, lo], axis=1), jnp.concatenate([got, got], axis=0)
        )
        out = a_ref[:, cols] + mm_square(split(r_ref[:, cols]), split(state))
        scaled = out * lax.rsqrt(jnp.mean(out * out, axis=-1, keepdims=True) + norm_floor)
        out_ref[:, cols] = (scaled * gate_ref[:, cols]).astype(bf16)


def output_kernel(masks, *refs):
    out_ref = refs[2 * masks]
    total = None
    for m in range(masks):
        part = dot(refs[m][...], refs[masks + m][...])
        total = part if total is None else total + part
    out_ref[...] = total.astype(bf16)


def xor_permute(value, mask):
    count = lax.axis_size("head")
    return lax.ppermute(value, "head", [(i, i ^ mask) for i in range(count)])


def gather_chunks(parts, masks):
    pieces = {0: list(parts)}
    top = masks // 2
    order = []
    while top >= 1:
        order.append(top)
        top //= 2
    for bit in order:
        for mask in sorted(pieces):
            pieces[mask | bit] = [xor_permute(c, bit) for c in pieces[mask]]
    return [pieces[m] for m in range(masks)]


def vmem_call(kernel, out_shape, operands, scalars=0, scratch=(), flops=0):
    specs = [
        pl.BlockSpec(memory_space=pltpu.SMEM if i < scalars else pltpu.VMEM)
        for i in range(len(operands))
    ]
    outs = jax.tree.map(lambda _: pl.BlockSpec(memory_space=pltpu.VMEM), out_shape)
    return pl.pallas_call(
        kernel,
        out_shape=out_shape,
        in_specs=specs,
        out_specs=outs,
        scratch_shapes=list(scratch),
        cost_estimate=pl.CostEstimate(flops=flops, transcendentals=0, bytes_accessed=flops // 256),
    )(*operands)


def on_device(
    layer_in,
    query_weight,
    key_weight,
    value_weight,
    gate_weight,
    beta_weight,
    decay_weight,
    conv_weight,
    decay_log,
    beta_bias,
    decay_bias,
    norm_gain,
    out_weight,
):
    tokens, features = layer_in.shape
    heads = beta_weight.shape[1]
    channels = query_weight.shape[1]
    dim = channels // heads
    taps = conv_weight.shape[0]
    masks = lax.axis_size("head")
    slabs = lax.axis_size("seq")
    blocks = tokens // BLOCK
    chunks = 2
    head = lax.axis_index("head")
    position = lax.axis_index("seq")
    head_at = head.reshape(1).astype(jnp.int32)
    pos_at = position.reshape(1).astype(jnp.int32)

    step = tokens // chunks
    x_pieces = gather_chunks([layer_in[c * step : (c + 1) * step] for c in range(chunks)], masks)
    tail = layer_in[tokens - HALO :]
    halos = []
    for mask in range(masks):
        pairs = [
            (s * masks + h, (s + 1) * masks + (h ^ mask))
            for s in range(slabs - 1)
            for h in range(masks)
        ]
        halos.append(lax.ppermute(tail, ("seq", "head"), pairs))

    lanes = 128
    narrow = jnp.concatenate([beta_weight, decay_weight], axis=1)
    narrow = jnp.pad(narrow, ((0, 0), (0, lanes - 2 * heads)))
    bias = jnp.pad(jnp.concatenate([beta_bias, decay_bias]), (0, lanes - 2 * heads))[None]
    rate = jnp.pad(jnp.exp(decay_log), (heads, lanes - 2 * heads))[None]
    conv = conv_weight.reshape(taps * 3, channels)
    gain = jnp.tile(norm_gain, heads)[None]

    x_flat = [c for piece in x_pieces for c in piece]
    shape = jax.ShapeDtypeStruct
    ext = pltpu.VMEM((tokens + HALO, channels), f32)
    keys, running, solved, prefix, slab, slab_low = vmem_call(
        functools.partial(key_kernel, masks, chunks, heads, dim, taps),
        (
            shape((tokens, channels), f32),
            shape((tokens, lanes), f32),
            shape((blocks * heads, BLOCK, 2 * dim), f32),
            shape(((blocks - 1) * heads, dim, 2 * dim), f32),
            shape((heads, dim, 2 * dim), f32),
            shape((heads, dim, 2 * dim), bf16),
        ),
        [head_at, *x_flat, *halos, key_weight, value_weight, narrow, conv, bias, rate],
        scalars=1,
        scratch=(ext,),
        flops=10**10,
    )

    width = out_weight.shape[1] // masks
    sends = [
        lax.dynamic_slice(out_weight, (0, (head ^ m) * width), (channels, width))
        for m in range(masks)
    ]
    sends, _ = lax.optimization_barrier((sends, x_pieces[masks // 2]))
    columns = [sends[0]] + [xor_permute(sends[m], m) for m in range(1, masks)]

    x_late, _ = lax.optimization_barrier((x_flat, slab_low))
    queries, gates = vmem_call(
        functools.partial(query_kernel, masks, chunks, heads, dim, taps),
        (shape((tokens, channels), f32), shape((tokens, channels), f32)),
        [head_at, *x_late, *halos, query_weight, gate_weight, conv, gain],
        scalars=1,
        scratch=(ext,),
        flops=4 * 10**9,
    )

    def shifted(value, distance):
        pairs = [(s, s + distance) for s in range(slabs - distance)]
        return lax.ppermute(value, "seq", pairs)

    before = None
    distance = 1
    local = reader = None
    while 2 * distance < slabs:
        got = shifted(slab_low, distance)
        maps = (heads, dim, 2 * dim)
        operands = [pos_at, got] + ([] if before is None else [before]) + [slab]
        before, slab, slab_low = vmem_call(
            functools.partial(step_kernel, heads, dim, before is None, distance),
            (shape(maps, f32), shape(maps, f32), shape(maps, bf16)),
            operands,
            scalars=1,
            flops=10**8,
        )
        distance *= 2
    got = shifted(slab_low[:, :, dim:], distance)
    local, reader = vmem_call(
        functools.partial(read_kernel, heads, dim),
        (shape((tokens, channels), f32), shape((tokens, channels), f32)),
        [queries, keys, running, solved, prefix],
        flops=4 * 10**9,
    )
    hidden = vmem_call(
        functools.partial(hidden_kernel, heads, dim),
        shape((tokens, channels), bf16),
        [local, reader, gates, before, got],
        flops=10**8,
    )
    pieces = gather_chunks([hidden], masks)
    return vmem_call(
        functools.partial(output_kernel, masks),
        shape((tokens, width), bf16),
        [p[0] for p in pieces] + columns,
        flops=10**9,
    )


def solution(mesh):
    return jax.shard_map(
        on_device,
        mesh=mesh,
        in_specs=(
            P("seq", "head"),
            P(None, "head"),
            P(None, "head"),
            P(None, "head"),
            P(None, "head"),
            P(None, "head"),
            P(None, "head"),
            P(None, None, "head"),
            P("head"),
            P("head"),
            P("head"),
            P(),
            P("head", None),
        ),
        out_specs=P("seq", "head"),
        check_vma=False,
    )
```

```python
import functools

import jax
import jax.numpy as jnp
from jax import lax
from jax.experimental import pallas as pl
from jax.experimental.pallas import tpu as pltpu
from jax.sharding import PartitionSpec as P

BLOCK = 128
HALO = 16
norm_floor = 0.0001
f32 = jnp.float32
bf16 = jnp.bfloat16


def split(a):
    hi = a.astype(bf16)
    return hi, (a - hi.astype(f32)).astype(bf16)


def dot(a, b):
    return lax.dot_general(a, b, (((1,), (0,)), ((), ())), preferred_element_type=f32)


def dot_nt(a, b):
    return lax.dot_general(a, b, (((1,), (1,)), ((), ())), preferred_element_type=f32)


def mm_square(a, b):
    n = b[0].shape[1]
    right = jnp.concatenate([b[0], b[1]], axis=1)
    out = dot(jnp.concatenate([a[0], a[1]], axis=1), jnp.concatenate([right, right], axis=0))
    return out[:, :n] + out[:, n:]


def mm_wide(a, b):
    left = jnp.concatenate([a[0], a[1]], axis=1)
    return dot(left, jnp.concatenate([b[0], b[0]], axis=0)) + dot(a[0], b[1])


def mm_nt(a, b):
    left = jnp.concatenate([a[0], a[1]], axis=1)
    return dot_nt(left, jnp.concatenate([b[0], b[0]], axis=1)) + dot_nt(a[0], b[1])


def iotas(n):
    return (
        lax.broadcasted_iota(jnp.int32, (n, n), 0),
        lax.broadcasted_iota(jnp.int32, (n, n), 1),
    )


def project(pieces, weight_ref, index, features):
    parts = []
    for chunk in range(len(pieces[0])):
        total = None
        for mask in range(len(pieces)):
            start = pl.multiple_of((index ^ mask) * features, features)
            part = dot(pieces[mask][chunk][...], weight_ref[pl.ds(start, features), :])
            total = part if total is None else total + part
        parts.append(total)
    return parts


def project_rows(pieces, weight_ref, index, features):
    parts = []
    for chunk in range(len(pieces[0])):
        total = None
        for mask in range(len(pieces)):
            start = pl.multiple_of((index ^ mask) * features, features)
            x = pieces[mask][chunk]
            x = x[pl.ds(HALO, x.shape[0] - HALO), :] if chunk == 0 else x[...]
            part = dot_nt(weight_ref[:, pl.ds(start, features)], x)
            total = part if total is None else total + part
        parts.append(total)
    return jnp.concatenate(parts, axis=1)


def conv_rows(ext_ref, raw, conv_ref, channel, taps, tokens):
    at = 0
    for part in raw:
        ext_ref[pl.ds(at, part.shape[0]), :] = part
        at += part.shape[0]
    summed = None
    for s in range(taps):
        part = conv_ref[channel, pl.ds(s, 1), :] * ext_ref[pl.ds(HALO - s, tokens), :]
        summed = part if summed is None else summed + part
    return jax.nn.silu(summed)


def unit_heads(values, heads, dim):
    parts = []
    for h in range(heads):
        v = values[:, h * dim : (h + 1) * dim]
        parts.append(v * lax.rsqrt(jnp.sum(v * v, axis=-1, keepdims=True) + 1.0))
    return jnp.concatenate(parts, axis=1)


def decay_of(running, running_t, unit):
    row, col = iotas(BLOCK)
    spread = running_t[:, unit : unit + 1] - running[unit : unit + 1, :]
    return jnp.where(row >= col, jnp.exp(jnp.minimum(spread, 0.0)), 0.0)


def take_pieces(refs, masks, chunks):
    return [[refs[m * chunks + c] for c in range(chunks)] for m in range(masks)]


def key_kernel(masks, chunks, heads, dim, taps, *refs):
    index = refs[0][0]
    decay_log, beta_bias, decay_bias = refs[1:4]
    refs = refs[4:]
    pieces = take_pieces(refs, masks, chunks)
    refs = refs[masks * chunks :]
    key_w, value_w, beta_w, decay_w, conv_ref = refs[:5]
    k_out, run_out, solved_out, prefix_out, slab_out, slab_low_out, ext = refs[5:]
    tokens = k_out.shape[0]
    features = pieces[0][0].shape[1]
    blocks = tokens // BLOCK
    units = [(b, h) for b in range(blocks) for h in range(heads)]
    row, col = iotas(BLOCK)
    eye = jnp.where(row == col, 1.0, 0.0).astype(f32)

    beta_raw = project_rows(pieces, beta_w, index, features)
    decay_raw = project_rows(pieces, decay_w, index, features)
    beta_rows, log_rows = [], []
    for h in range(heads):
        beta_rows.append(jax.nn.sigmoid(beta_raw[h : h + 1] + beta_bias[h]))
        z = decay_raw[h : h + 1] + decay_bias[h]
        soft = jnp.maximum(z, 0.0) + jnp.log(1.0 + jnp.exp(-jnp.abs(z)))
        log_rows.append(-jnp.exp(jnp.full_like(z, decay_log[h])) * soft)

    def by_unit(rows):
        return jnp.concatenate(
            [rows[h][:, b * BLOCK : (b + 1) * BLOCK] for b, h in units], axis=0
        )

    running = lax.dot_general(
        by_unit(log_rows),
        jnp.where(row <= col, 1.0, 0.0).astype(f32),
        (((1,), (0,)), ((), ())),
        preferred_element_type=f32,
        precision=lax.Precision.HIGHEST,
    )
    run_out[...] = running
    running_t = jnp.transpose(running)
    beta_t = jnp.transpose(by_unit(beta_rows))
    keys = unit_heads(
        conv_rows(ext, project(pieces, key_w, index, features), conv_ref, 1, taps, tokens),
        heads,
        dim,
    )
    k_out[...] = keys
    values = conv_rows(
        ext, project(pieces, value_w, index, features), conv_ref, 2, taps, tokens
    )
    k_of = {}
    lower = {}
    inverse = {}
    for b, h in units:
        k = keys[b * BLOCK : (b + 1) * BLOCK, h * dim : (h + 1) * dim]
        k_of[b, h] = k
        pair = split(k)
        unit = b * heads + h
        gram = mm_nt(pair, pair)
        system = jnp.where(
            row > col,
            beta_t[:, unit : unit + 1] * decay_of(running, running_t, unit) * gram,
            0.0,
        )
        lower[b, h] = system
        link = (row // 2 == col // 2) & (row > col)
        inverse[b, h] = eye - jnp.where(link, system, 0.0)
    width = 2
    while width < BLOCK:
        link = (row // (2 * width) == col // (2 * width)) & (row // width > col // width)
        middle = {}
        pairs = {}
        for u in units:
            pairs[u] = split(inverse[u])
            middle[u] = mm_square(split(jnp.where(link, lower[u], 0.0)), pairs[u])
        for u in units:
            inverse[u] = inverse[u] - mm_square(pairs[u], split(middle[u]))
        width *= 2
    maps = {}
    solved_pair = {}
    for b, h in units:
        k = k_of[b, h]
        unit = b * heads + h
        bcol = beta_t[:, unit : unit + 1]
        rcol = running_t[:, unit : unit + 1]
        v = values[b * BLOCK : (b + 1) * BLOCK, h * dim : (h + 1) * dim]
        right = jnp.concatenate([(bcol * jnp.exp(rcol)) * k, bcol * v], axis=1)
        solved = mm_wide(split(inverse[b, h]), split(right))
        solved_out[b * heads + h] = solved
        solved_pair[b, h] = split(solved)
    for b, h in units:
        rcol = running_t[:, b * heads + h : b * heads + h + 1]
        last = rcol[BLOCK - 1 : BLOCK, :]
        weighted = jnp.transpose(jnp.exp(last - rcol) * k_of[b, h])
        moved = mm_wide(split(weighted), solved_pair[b, h])
        transit = jnp.exp(last) * eye - moved[:, :dim]
        maps[b, h] = jnp.concatenate([transit, moved[:, dim:]], axis=1)

    def compose(later, earlier):
        out = mm_wide(split(later[:, :dim]), split(earlier))
        return jnp.concatenate([out[:, :dim], out[:, dim:] + later[:, dim:]], axis=1)

    for h in range(heads):
        spans = {(b, 1): maps[b, h] for b in range(blocks)}

        def span(start, count):
            if (start, count) not in spans:
                half = 1
                while half * 2 < count:
                    half *= 2
                spans[start, count] = compose(
                    span(start + half, count - half), span(start, half)
                )
            return spans[start, count]

        for b in range(1, blocks):
            prefix_out[h * (blocks - 1) + b - 1] = span(0, b)
        slab = span(0, blocks)
        slab_out[h] = slab
        slab_low_out[h] = slab.astype(bf16)


def query_kernel(masks, chunks, heads, dim, taps, *refs):
    index = refs[0][0]
    refs = refs[1:]
    pieces = take_pieces(refs, masks, chunks)
    query_w, gate_w, conv_ref, gain_ref = refs[masks * chunks : masks * chunks + 4]
    q_out, gate_out, ext = refs[masks * chunks + 4 :]
    tokens = q_out.shape[0]
    features = pieces[0][0].shape[1]
    raw = project(pieces, query_w, index, features)
    q_out[...] = unit_heads(conv_rows(ext, raw, conv_ref, 0, taps, tokens), heads, dim)
    gain = jnp.concatenate([gain_ref[...]] * heads, axis=1)
    at = 0
    for chunk, part in enumerate(project(pieces, gate_w, index, features)):
        part = part[HALO:] if chunk == 0 else part
        gate_out[pl.ds(at, part.shape[0]), :] = jax.nn.silu(part) * gain
        at += part.shape[0]


def read_kernel(heads, dim, q_ref, k_ref, run_ref, solved_ref, prefix_ref, a_out, r_out):
    tokens = q_ref.shape[0]
    blocks = tokens // BLOCK
    units = [(b, h) for b in range(blocks) for h in range(heads)]
    running = run_ref[...]
    running_t = jnp.transpose(running)
    mixing = {}
    for b, h in units:
        q = split(q_ref[pl.ds(b * BLOCK, BLOCK), pl.ds(h * dim, dim)])
        k = split(k_ref[pl.ds(b * BLOCK, BLOCK), pl.ds(h * dim, dim)])
        mixing[b, h] = decay_of(running, running_t, b * heads + h) * mm_nt(q, k)
    for b, h in units:
        rows, cols = pl.ds(b * BLOCK, BLOCK), pl.ds(h * dim, dim)
        out = mm_wide(split(mixing[b, h]), split(solved_ref[b * heads + h]))
        growth = jnp.exp(running_t[:, b * heads + h : b * heads + h + 1])
        reader = growth * q_ref[rows, cols] - out[:, :dim]
        local = out[:, dim:]
        if b > 0:
            moved = mm_wide(split(reader), split(prefix_ref[h * (blocks - 1) + b - 1]))
            reader = moved[:, :dim]
            local = local + moved[:, dim:]
        a_out[rows, cols] = local
        r_out[rows, cols] = reader


def step_kernel(heads, dim, first, distance, pos_ref, got_ref, *refs):
    if first:
        own_ref, before_out, own_out, low_out = refs
    else:
        before_ref, own_ref, before_out, own_out, low_out = refs
    valid = pos_ref[0] >= distance
    row = lax.broadcasted_iota(jnp.int32, (dim, 2 * dim), 0)
    col = lax.broadcasted_iota(jnp.int32, (dim, 2 * dim), 1)
    unchanged = jnp.where(row == col, 1.0, 0.0).astype(f32)
    for h in range(heads):
        got = jnp.where(valid, got_ref[h].astype(f32), unchanged)
        low = got.astype(bf16)
        low = jnp.concatenate([low, low], axis=0)

        def after(later):
            hi, lo = split(later[:, :dim])
            out = dot(jnp.concatenate([hi, lo], axis=1), low)
            return jnp.concatenate([out[:, :dim], out[:, dim:] + later[:, dim:]], axis=1)

        own = after(own_ref[h])
        own_out[h] = own
        low_out[h] = own.astype(bf16)
        before_out[h] = got if first else after(before_ref[h])


def hidden_kernel(heads, dim, a_ref, r_ref, gate_ref, before_ref, got_ref, out_ref):
    for h in range(heads):
        cols = pl.ds(h * dim, dim)
        before = before_ref[h]
        got = got_ref[h]
        hi, lo = split(before[:, :dim])
        state = before[:, dim:] + dot(
            jnp.concatenate([hi, lo], axis=1), jnp.concatenate([got, got], axis=0)
        )
        out = a_ref[:, cols] + mm_square(split(r_ref[:, cols]), split(state))
        scaled = out * lax.rsqrt(jnp.mean(out * out, axis=-1, keepdims=True) + norm_floor)
        out_ref[:, cols] = (scaled * gate_ref[:, cols]).astype(bf16)


def output_kernel(masks, *refs):
    out_ref = refs[2 * masks]
    total = None
    for m in range(masks):
        part = dot(refs[m][...], refs[masks + m][...])
        total = part if total is None else total + part
    out_ref[...] = total.astype(bf16)


def xor_permute(value, mask):
    count = lax.axis_size("head")
    return lax.ppermute(value, "head", [(i, i ^ mask) for i in range(count)])


def gather_chunks(parts, masks):
    order = []
    bit = masks // 2
    while bit >= 1:
        order.append(bit)
        bit //= 2
    pieces = {0: list(parts)}
    for bit in order:
        for mask in sorted(pieces):
            got = list(pieces[mask])
            for c in reversed(range(len(got))):
                got[c] = xor_permute(got[c], bit)
            pieces[mask | bit] = got
    return [pieces[m] for m in range(masks)]


def vmem_call(kernel, out_shape, operands, scalars=0, scratch=(), limit=16):
    specs = [
        pl.BlockSpec(memory_space=pltpu.SMEM if i < scalars else pltpu.VMEM)
        for i in range(len(operands))
    ]
    outs = jax.tree.map(lambda _: pl.BlockSpec(memory_space=pltpu.VMEM), out_shape)
    return pl.pallas_call(
        kernel,
        out_shape=out_shape,
        in_specs=specs,
        out_specs=outs,
        scratch_shapes=list(scratch),
        compiler_params=pltpu.CompilerParams(vmem_limit_bytes=limit * 2**20),
    )(*operands)


def on_device(
    layer_in,
    query_weight,
    key_weight,
    value_weight,
    gate_weight,
    beta_weight,
    decay_weight,
    conv_weight,
    decay_log,
    beta_bias,
    decay_bias,
    norm_gain,
    out_weight,
):
    tokens, _ = layer_in.shape
    heads = beta_weight.shape[1]
    channels = query_weight.shape[1]
    dim = channels // heads
    taps = conv_weight.shape[0]
    masks = lax.axis_size("head")
    slabs = lax.axis_size("seq")
    blocks = tokens // BLOCK
    head = lax.axis_index("head")
    head_at = head.reshape(1).astype(jnp.int32)
    pos_at = lax.axis_index("seq").reshape(1).astype(jnp.int32)

    def shifted(value, distance):
        pairs = [(s, s + distance) for s in range(slabs - distance)]
        return lax.ppermute(value, "seq", pairs)

    chunks = 2
    step = tokens // chunks
    halo = shifted(layer_in[tokens - HALO :], 1)
    first = jnp.concatenate([halo, layer_in[:step]], axis=0)
    x_pieces = gather_chunks([first, layer_in[step:]], masks)
    x_flat = [c for piece in x_pieces for c in piece]
    conv = conv_weight.transpose(1, 0, 2)
    gain = norm_gain[None]

    shape = jax.ShapeDtypeStruct
    ext = pltpu.VMEM((tokens + HALO, channels), f32)
    maps = (heads, dim, 2 * dim)
    rows = (tokens, channels)
    keys, running, solved, prefix, slab, slab_low = vmem_call(
        functools.partial(key_kernel, masks, chunks, heads, dim, taps),
        (
            shape(rows, f32),
            shape((blocks * heads, BLOCK), f32),
            shape((blocks * heads, BLOCK, 2 * dim), f32),
            shape(((blocks - 1) * heads, dim, 2 * dim), f32),
            shape(maps, f32),
            shape(maps, bf16),
        ),
        [head_at, decay_log, beta_bias, decay_bias, *x_flat]
        + [key_weight, value_weight, beta_weight.T, decay_weight.T, conv],
        scalars=4,
        scratch=(ext,),
        limit=24,
    )

    width = out_weight.shape[1] // masks
    sends = [
        lax.dynamic_slice(out_weight, (0, (head ^ m) * width), (channels, width))
        for m in range(masks)
    ]
    columns = [sends[0]]
    held, _ = lax.optimization_barrier((sends, x_pieces[masks // 2]))
    for m in range(1, masks):
        columns.append(xor_permute(held[m], m))

    x_late, _ = lax.optimization_barrier((x_flat, slab_low))
    queries, gates = vmem_call(
        functools.partial(query_kernel, masks, chunks, heads, dim, taps),
        (shape(rows, f32), shape(rows, f32)),
        [head_at, *x_late, query_weight, gate_weight, conv, gain],
        scalars=1,
        scratch=(ext,),
        limit=16,
    )

    before = None
    distance = 1
    while 2 * distance < slabs:
        got = shifted(slab_low, distance)
        operands = [pos_at, got] + ([] if before is None else [before]) + [slab]
        before, slab, slab_low = vmem_call(
            functools.partial(step_kernel, heads, dim, before is None, distance),
            (shape(maps, f32), shape(maps, f32), shape(maps, bf16)),
            operands,
            scalars=1,
            limit=8,
        )
        distance *= 2
    got = shifted(slab_low[:, :, dim:], distance)
    local, reader = vmem_call(
        functools.partial(read_kernel, heads, dim),
        (shape(rows, f32), shape(rows, f32)),
        [queries, keys, running, solved, prefix],
        limit=16,
    )
    hidden = vmem_call(
        functools.partial(hidden_kernel, heads, dim),
        shape(rows, bf16),
        [local, reader, gates, before, got],
        limit=8,
    )
    pieces = gather_chunks([hidden], masks)
    return vmem_call(
        functools.partial(output_kernel, masks),
        shape((tokens, width), bf16),
        [p[0] for p in pieces] + columns,
        limit=8,
    )


def solution(mesh):
    return jax.shard_map(
        on_device,
        mesh=mesh,
        in_specs=(
            P("seq", "head"),
            P(None, "head"),
            P(None, "head"),
            P(None, "head"),
            P(None, "head"),
            P(None, "head"),
            P(None, "head"),
            P(None, None, "head"),
            P("head"),
            P("head"),
            P("head"),
            P(),
            P("head", None),
        ),
        out_specs=P("seq", "head"),
        check_vma=False,
    )
```

```python
import functools

import jax
import jax.numpy as jnp
from jax import lax
from jax.experimental import pallas as pl
from jax.experimental.pallas import tpu as pltpu
from jax.sharding import PartitionSpec as P

BLOCK = 128
HALO = 16
norm_floor = 0.0001
f32 = jnp.float32
bf16 = jnp.bfloat16


def split(a):
    hi = a.astype(bf16)
    return hi, (a - hi.astype(f32)).astype(bf16)


def dot(a, b):
    return lax.dot_general(a, b, (((1,), (0,)), ((), ())), preferred_element_type=f32)


def dot_nt(a, b):
    return lax.dot_general(a, b, (((1,), (1,)), ((), ())), preferred_element_type=f32)


def mm_square(a, b):
    n = b[0].shape[1]
    right = jnp.concatenate([b[0], b[1]], axis=1)
    out = dot(jnp.concatenate([a[0], a[1]], axis=1), jnp.concatenate([right, right], axis=0))
    return out[:, :n] + out[:, n:]


def mm_wide(a, b):
    left = jnp.concatenate([a[0], a[1]], axis=1)
    return dot(left, jnp.concatenate([b[0], b[0]], axis=0)) + dot(a[0], b[1])


def mm_nt(a, b):
    left = jnp.concatenate([a[0], a[1]], axis=1)
    return dot_nt(left, jnp.concatenate([b[0], b[0]], axis=1)) + dot_nt(a[0], b[1])


def iotas(n):
    return (
        lax.broadcasted_iota(jnp.int32, (n, n), 0),
        lax.broadcasted_iota(jnp.int32, (n, n), 1),
    )


def project(pieces, weight_ref, index, features):
    parts = []
    for chunk in range(len(pieces[0])):
        total = None
        for mask in range(len(pieces)):
            start = pl.multiple_of((index ^ mask) * features, features)
            part = dot(pieces[mask][chunk][...], weight_ref[pl.ds(start, features), :])
            total = part if total is None else total + part
        parts.append(total)
    return parts


def project_rows(pieces, weight_ref, index, features):
    parts = []
    for chunk in range(len(pieces[0])):
        total = None
        for mask in range(len(pieces)):
            start = pl.multiple_of((index ^ mask) * features, features)
            x = pieces[mask][chunk]
            x = x[pl.ds(HALO, x.shape[0] - HALO), :] if chunk == 0 else x[...]
            part = dot_nt(weight_ref[:, pl.ds(start, features)], x)
            total = part if total is None else total + part
        parts.append(total)
    return jnp.concatenate(parts, axis=1)


def conv_rows(ext_ref, raw, conv_ref, channel, taps, tokens):
    at = 0
    for part in raw:
        ext_ref[pl.ds(at, part.shape[0]), :] = part
        at += part.shape[0]
    summed = None
    for s in range(taps):
        part = conv_ref[channel, pl.ds(s, 1), :] * ext_ref[pl.ds(HALO - s, tokens), :]
        summed = part if summed is None else summed + part
    return jax.nn.silu(summed)


def unit_heads(values, heads, dim):
    parts = []
    for h in range(heads):
        v = values[:, h * dim : (h + 1) * dim]
        parts.append(v * lax.rsqrt(jnp.sum(v * v, axis=-1, keepdims=True) + 1.0))
    return jnp.concatenate(parts, axis=1)


def decay_of(running, running_t, unit):
    row, col = iotas(BLOCK)
    spread = running_t[:, unit : unit + 1] - running[unit : unit + 1, :]
    return jnp.where(row >= col, jnp.exp(jnp.minimum(spread, 0.0)), 0.0)


def take_pieces(refs, masks, chunks):
    return [[refs[m * chunks + c] for c in range(chunks)] for m in range(masks)]


def key_kernel(masks, chunks, heads, dim, taps, *refs):
    index = refs[0][0]
    decay_log, beta_bias, decay_bias = refs[1:4]
    refs = refs[4:]
    pieces = take_pieces(refs, masks, chunks)
    refs = refs[masks * chunks :]
    key_w, value_w, beta_w, decay_w, conv_ref = refs[:5]
    k_hbm, run_out, solved_hbm, prefix_hbm, slab_hbm, slab_low_out = refs[5:11]
    ext, k_out, solved_out, prefix_out, slab_out, sems = refs[11:]
    tokens = k_out.shape[0]
    leaving = [
        pltpu.make_async_copy(k_out, k_hbm, sems.at[0]),
        pltpu.make_async_copy(solved_out, solved_hbm, sems.at[1]),
        pltpu.make_async_copy(prefix_out, prefix_hbm, sems.at[2]),
        pltpu.make_async_copy(slab_out, slab_hbm, sems.at[3]),
    ]
    features = pieces[0][0].shape[1]
    blocks = tokens // BLOCK
    units = [(b, h) for b in range(blocks) for h in range(heads)]
    row, col = iotas(BLOCK)
    eye = jnp.where(row == col, 1.0, 0.0).astype(f32)

    beta_raw = project_rows(pieces, beta_w, index, features)
    decay_raw = project_rows(pieces, decay_w, index, features)
    beta_rows, log_rows = [], []
    for h in range(heads):
        beta_rows.append(jax.nn.sigmoid(beta_raw[h : h + 1] + beta_bias[h]))
        z = decay_raw[h : h + 1] + decay_bias[h]
        soft = jnp.maximum(z, 0.0) + jnp.log(1.0 + jnp.exp(-jnp.abs(z)))
        log_rows.append(-jnp.exp(jnp.full_like(z, decay_log[h])) * soft)

    def by_unit(rows):
        return jnp.concatenate(
            [rows[h][:, b * BLOCK : (b + 1) * BLOCK] for b, h in units], axis=0
        )

    running = lax.dot_general(
        by_unit(log_rows),
        jnp.where(row <= col, 1.0, 0.0).astype(f32),
        (((1,), (0,)), ((), ())),
        preferred_element_type=f32,
        precision=lax.Precision.HIGHEST,
    )
    run_out[...] = running
    running_t = jnp.transpose(running)
    beta_t = jnp.transpose(by_unit(beta_rows))
    keys = unit_heads(
        conv_rows(ext, project(pieces, key_w, index, features), conv_ref, 1, taps, tokens),
        heads,
        dim,
    )
    k_out[...] = keys
    leaving[0].start()
    values = conv_rows(
        ext, project(pieces, value_w, index, features), conv_ref, 2, taps, tokens
    )
    k_of = {}
    lower = {}
    inverse = {}
    for b, h in units:
        k = keys[b * BLOCK : (b + 1) * BLOCK, h * dim : (h + 1) * dim]
        k_of[b, h] = k
        pair = split(k)
        unit = b * heads + h
        gram = mm_nt(pair, pair)
        system = jnp.where(
            row > col,
            beta_t[:, unit : unit + 1] * decay_of(running, running_t, unit) * gram,
            0.0,
        )
        lower[b, h] = system
        link = (row // 2 == col // 2) & (row > col)
        inverse[b, h] = eye - jnp.where(link, system, 0.0)
    width = 2
    while width < BLOCK:
        link = (row // (2 * width) == col // (2 * width)) & (row // width > col // width)
        middle = {}
        pairs = {}
        for u in units:
            pairs[u] = split(inverse[u])
            middle[u] = mm_square(split(jnp.where(link, lower[u], 0.0)), pairs[u])
        for u in units:
            inverse[u] = inverse[u] - mm_square(pairs[u], split(middle[u]))
        width *= 2
    maps = {}
    solved_pair = {}
    for b, h in units:
        k = k_of[b, h]
        unit = b * heads + h
        bcol = beta_t[:, unit : unit + 1]
        rcol = running_t[:, unit : unit + 1]
        v = values[b * BLOCK : (b + 1) * BLOCK, h * dim : (h + 1) * dim]
        right = jnp.concatenate([(bcol * jnp.exp(rcol)) * k, bcol * v], axis=1)
        solved = mm_wide(split(inverse[b, h]), split(right))
        solved_out[b * heads + h] = solved
        solved_pair[b, h] = split(solved)
    leaving[1].start()
    for b, h in units:
        rcol = running_t[:, b * heads + h : b * heads + h + 1]
        last = rcol[BLOCK - 1 : BLOCK, :]
        weighted = jnp.transpose(jnp.exp(last - rcol) * k_of[b, h])
        moved = mm_wide(split(weighted), solved_pair[b, h])
        transit = jnp.exp(last) * eye - moved[:, :dim]
        maps[b, h] = jnp.concatenate([transit, moved[:, dim:]], axis=1)

    def compose(later, earlier):
        out = mm_wide(split(later[:, :dim]), split(earlier))
        return jnp.concatenate([out[:, :dim], out[:, dim:] + later[:, dim:]], axis=1)

    slabs = []
    for h in range(heads):
        spans = {(b, 1): maps[b, h] for b in range(blocks)}

        def span(start, count, h=h, spans=spans):
            if (start, count) not in spans:
                half = 1
                while half * 2 < count:
                    half *= 2
                spans[start, count] = compose(
                    span(start + half, count - half), span(start, half)
                )
            return spans[start, count]

        for b in range(1, blocks):
            prefix_out[h * (blocks - 1) + b - 1] = span(0, b)
        slabs.append(span)
    leaving[2].start()
    for h, span in enumerate(slabs):
        slab = span(0, blocks)
        slab_out[h] = slab
        slab_low_out[h] = slab.astype(bf16)
    leaving[3].start()
    for copy in leaving:
        copy.wait()


def query_kernel(masks, chunks, heads, dim, taps, *refs):
    index = refs[0][0]
    refs = refs[1:]
    pieces = take_pieces(refs, masks, chunks)
    query_w, gate_w, conv_ref, gain_ref = refs[masks * chunks : masks * chunks + 4]
    q_out, gate_out, ext = refs[masks * chunks + 4 :]
    tokens = q_out.shape[0]
    features = pieces[0][0].shape[1]
    raw = project(pieces, query_w, index, features)
    q_out[...] = unit_heads(conv_rows(ext, raw, conv_ref, 0, taps, tokens), heads, dim)
    gain = jnp.concatenate([gain_ref[...]] * heads, axis=1)
    at = 0
    for chunk, part in enumerate(project(pieces, gate_w, index, features)):
        part = part[HALO:] if chunk == 0 else part
        gate_out[pl.ds(at, part.shape[0]), :] = jax.nn.silu(part) * gain
        at += part.shape[0]


def read_kernel(heads, dim, q_ref, k_ref, run_ref, solved_ref, prefix_ref, a_out, r_out):
    tokens = q_ref.shape[0]
    blocks = tokens // BLOCK
    units = [(b, h) for b in range(blocks) for h in range(heads)]
    running = run_ref[...]
    running_t = jnp.transpose(running)
    mixing = {}
    for b, h in units:
        q = split(q_ref[pl.ds(b * BLOCK, BLOCK), pl.ds(h * dim, dim)])
        k = split(k_ref[pl.ds(b * BLOCK, BLOCK), pl.ds(h * dim, dim)])
        mixing[b, h] = decay_of(running, running_t, b * heads + h) * mm_nt(q, k)
    for b, h in units:
        rows, cols = pl.ds(b * BLOCK, BLOCK), pl.ds(h * dim, dim)
        out = mm_wide(split(mixing[b, h]), split(solved_ref[b * heads + h]))
        growth = jnp.exp(running_t[:, b * heads + h : b * heads + h + 1])
        reader = growth * q_ref[rows, cols] - out[:, :dim]
        local = out[:, dim:]
        if b > 0:
            moved = mm_wide(split(reader), split(prefix_ref[h * (blocks - 1) + b - 1]))
            reader = moved[:, :dim]
            local = local + moved[:, dim:]
        a_out[rows, cols] = local
        r_out[rows, cols] = reader


def step_kernel(heads, dim, first, distance, pos_ref, got_ref, *refs):
    if first:
        own_ref, before_out, own_out, low_out = refs
    else:
        before_ref, own_ref, before_out, own_out, low_out = refs
    valid = pos_ref[0] >= distance
    row = lax.broadcasted_iota(jnp.int32, (dim, 2 * dim), 0)
    col = lax.broadcasted_iota(jnp.int32, (dim, 2 * dim), 1)
    unchanged = jnp.where(row == col, 1.0, 0.0).astype(f32)
    for h in range(heads):
        got = jnp.where(valid, got_ref[h].astype(f32), unchanged)
        low = got.astype(bf16)
        low = jnp.concatenate([low, low], axis=0)

        def after(later):
            hi, lo = split(later[:, :dim])
            out = dot(jnp.concatenate([hi, lo], axis=1), low)
            return jnp.concatenate([out[:, :dim], out[:, dim:] + later[:, dim:]], axis=1)

        own = after(own_ref[h])
        own_out[h] = own
        low_out[h] = own.astype(bf16)
        before_out[h] = got if first else after(before_ref[h])


def hidden_kernel(heads, dim, a_ref, r_ref, gate_ref, before_ref, got_ref, out_ref):
    for h in range(heads):
        cols = pl.ds(h * dim, dim)
        before = before_ref[h]
        got = got_ref[h]
        hi, lo = split(before[:, :dim])
        state = before[:, dim:] + dot(
            jnp.concatenate([hi, lo], axis=1), jnp.concatenate([got, got], axis=0)
        )
        out = a_ref[:, cols] + mm_square(split(r_ref[:, cols]), split(state))
        scaled = out * lax.rsqrt(jnp.mean(out * out, axis=-1, keepdims=True) + norm_floor)
        out_ref[:, cols] = (scaled * gate_ref[:, cols]).astype(bf16)


def output_kernel(count, has_sum, *refs):
    out_ref = refs[-1]
    total = refs[2 * count][...] if has_sum else None
    for m in range(count):
        part = dot(refs[m][...], refs[count + m][...])
        total = part if total is None else total + part
    out_ref[...] = total.astype(out_ref.dtype)


def xor_permute(value, mask):
    count = lax.axis_size("head")
    return lax.ppermute(value, "head", [(i, i ^ mask) for i in range(count)])


def gather_chunks(parts, masks):
    order = []
    bit = masks // 2
    while bit >= 1:
        order.append(bit)
        bit //= 2
    pieces = {0: list(parts)}
    for bit in order:
        for mask in sorted(pieces):
            got = list(pieces[mask])
            for c in reversed(range(len(got))):
                got[c] = xor_permute(got[c], bit)
            pieces[mask | bit] = got
    return [pieces[m] for m in range(masks)]


def vmem_call(kernel, out_shape, operands, scalars=0, scratch=(), limit=16, hbm=()):
    specs = [
        pl.BlockSpec(memory_space=pltpu.SMEM if i < scalars else pltpu.VMEM)
        for i in range(len(operands))
    ]
    outs = pl.BlockSpec(memory_space=pltpu.VMEM)
    if isinstance(out_shape, tuple):
        outs = tuple(
            pl.BlockSpec(memory_space=pltpu.HBM if i in hbm else pltpu.VMEM)
            for i in range(len(out_shape))
        )
        out_shape = tuple(
            pltpu.HBM(o.shape, o.dtype) if i in hbm else o for i, o in enumerate(out_shape)
        )
    return pl.pallas_call(
        kernel,
        out_shape=out_shape,
        in_specs=specs,
        out_specs=outs,
        scratch_shapes=list(scratch),
        compiler_params=pltpu.CompilerParams(vmem_limit_bytes=limit * 2**20),
    )(*operands)


def on_device(
    layer_in,
    query_weight,
    key_weight,
    value_weight,
    gate_weight,
    beta_weight,
    decay_weight,
    conv_weight,
    decay_log,
    beta_bias,
    decay_bias,
    norm_gain,
    out_weight,
):
    tokens, _ = layer_in.shape
    heads = beta_weight.shape[1]
    channels = query_weight.shape[1]
    dim = channels // heads
    taps = conv_weight.shape[0]
    masks = lax.axis_size("head")
    slabs = lax.axis_size("seq")
    blocks = tokens // BLOCK
    head = lax.axis_index("head")
    head_at = head.reshape(1).astype(jnp.int32)
    pos_at = lax.axis_index("seq").reshape(1).astype(jnp.int32)

    def shifted(value, distance):
        pairs = [(s, s + distance) for s in range(slabs - distance)]
        return lax.ppermute(value, "seq", pairs)

    chunks = 2
    step = tokens // chunks
    halo = shifted(layer_in[tokens - HALO :], 1)
    first = jnp.concatenate([halo, layer_in[:step]], axis=0)
    x_pieces = gather_chunks([first, layer_in[step:]], masks)
    x_flat = [c for piece in x_pieces for c in piece]
    conv = conv_weight.transpose(1, 0, 2)
    gain = norm_gain[None]

    shape = jax.ShapeDtypeStruct
    ext = pltpu.VMEM((tokens + HALO, channels), f32)
    maps = (heads, dim, 2 * dim)
    rows = (tokens, channels)
    keys, running, solved, prefix, slab, slab_low = vmem_call(
        functools.partial(key_kernel, masks, chunks, heads, dim, taps),
        (
            shape(rows, f32),
            shape((blocks * heads, BLOCK), f32),
            shape((blocks * heads, BLOCK, 2 * dim), f32),
            shape(((blocks - 1) * heads, dim, 2 * dim), f32),
            shape(maps, f32),
            shape(maps, bf16),
        ),
        [head_at, decay_log, beta_bias, decay_bias, *x_flat]
        + [key_weight, value_weight, beta_weight.T, decay_weight.T, conv],
        scalars=4,
        scratch=(
            ext,
            pltpu.VMEM(rows, f32),
            pltpu.VMEM((blocks * heads, BLOCK, 2 * dim), f32),
            pltpu.VMEM(((blocks - 1) * heads, dim, 2 * dim), f32),
            pltpu.VMEM(maps, f32),
            pltpu.SemaphoreType.DMA((4,)),
        ),
        limit=24,
        hbm=(0, 2, 3, 4),
    )

    width = out_weight.shape[1] // masks
    sends = [
        lax.dynamic_slice(out_weight, (0, (head ^ m) * width), (channels, width))
        for m in range(masks)
    ]
    columns = [sends[0]]
    held, _ = lax.optimization_barrier((sends, x_pieces[masks // 2]))
    for m in range(1, masks):
        columns.append(xor_permute(held[m], m))

    x_late, _ = lax.optimization_barrier((x_flat, slab_low))
    queries, gates = vmem_call(
        functools.partial(query_kernel, masks, chunks, heads, dim, taps),
        (shape(rows, f32), shape(rows, f32)),
        [head_at, *x_late, query_weight, gate_weight, conv, gain],
        scalars=1,
        scratch=(ext,),
        limit=16,
    )

    before = None
    distance = 1
    while 2 * distance < slabs:
        got = shifted(slab_low, distance)
        operands = [pos_at, got] + ([] if before is None else [before]) + [slab]
        before, slab, slab_low = vmem_call(
            functools.partial(step_kernel, heads, dim, before is None, distance),
            (shape(maps, f32), shape(maps, f32), shape(maps, bf16)),
            operands,
            scalars=1,
            limit=8,
        )
        distance *= 2
    got = shifted(slab_low[:, :, dim:], distance)
    local, reader = vmem_call(
        functools.partial(read_kernel, heads, dim),
        (shape(rows, f32), shape(rows, f32)),
        [queries, keys, running, solved, prefix],
        limit=16,
    )
    hidden = vmem_call(
        functools.partial(hidden_kernel, heads, dim),
        shape(rows, bf16),
        [local, reader, gates, before, got],
        limit=8,
    )
    pieces = gather_chunks([hidden], masks)
    total = None
    stages = [list(range(masks // 2))] + [[m] for m in range(masks // 2, masks)]
    for i, stage in enumerate(stages):
        last = i == len(stages) - 1
        operands = [pieces[m][0] for m in stage] + [columns[m] for m in stage]
        total = vmem_call(
            functools.partial(output_kernel, len(stage), i > 0),
            shape((tokens, width), bf16 if last else f32),
            operands + ([total] if i > 0 else []),
            limit=8,
        )
    return total


def solution(mesh):
    return jax.shard_map(
        on_device,
        mesh=mesh,
        in_specs=(
            P("seq", "head"),
            P(None, "head"),
            P(None, "head"),
            P(None, "head"),
            P(None, "head"),
            P(None, "head"),
            P(None, "head"),
            P(None, None, "head"),
            P("head"),
            P("head"),
            P("head"),
            P(),
            P("head", None),
        ),
        out_specs=P("seq", "head"),
        check_vma=False,
    )
```

```python
import functools

import jax
import jax.numpy as jnp
from jax import lax
from jax.experimental import pallas as pl
from jax.experimental.pallas import tpu as pltpu
from jax.sharding import PartitionSpec as P

BLOCK = 128
HALO = 16
norm_floor = 0.0001
f32 = jnp.float32
bf16 = jnp.bfloat16


def split(a):
    hi = a.astype(bf16)
    return hi, (a - hi.astype(f32)).astype(bf16)


def dot(a, b):
    return lax.dot_general(a, b, (((1,), (0,)), ((), ())), preferred_element_type=f32)


def dot_nt(a, b):
    return lax.dot_general(a, b, (((1,), (1,)), ((), ())), preferred_element_type=f32)


def mm_square(a, b):
    n = b[0].shape[1]
    right = jnp.concatenate([b[0], b[1]], axis=1)
    out = dot(jnp.concatenate([a[0], a[1]], axis=1), jnp.concatenate([right, right], axis=0))
    return out[:, :n] + out[:, n:]


def mm_wide(a, b):
    left = jnp.concatenate([a[0], a[1]], axis=1)
    return dot(left, jnp.concatenate([b[0], b[0]], axis=0)) + dot(a[0], b[1])


def mm_nt(a, b):
    left = jnp.concatenate([a[0], a[1]], axis=1)
    return dot_nt(left, jnp.concatenate([b[0], b[0]], axis=1)) + dot_nt(a[0], b[1])


def iotas(n):
    return (
        lax.broadcasted_iota(jnp.int32, (n, n), 0),
        lax.broadcasted_iota(jnp.int32, (n, n), 1),
    )


def project(pieces, weight_ref, index, features):
    parts = []
    for chunk in range(len(pieces[0])):
        total = None
        for mask in range(len(pieces)):
            start = pl.multiple_of((index ^ mask) * features, features)
            part = dot(pieces[mask][chunk][...], weight_ref[pl.ds(start, features), :])
            total = part if total is None else total + part
        parts.append(total)
    return parts


def project_rows(pieces, weight_ref, index, features):
    parts = []
    for chunk in range(len(pieces[0])):
        total = None
        for mask in range(len(pieces)):
            start = pl.multiple_of((index ^ mask) * features, features)
            x = pieces[mask][chunk]
            x = x[pl.ds(HALO, x.shape[0] - HALO), :] if chunk == 0 else x[...]
            part = dot_nt(weight_ref[:, pl.ds(start, features)], x)
            total = part if total is None else total + part
        parts.append(total)
    return jnp.concatenate(parts, axis=1)


def conv_rows(ext_ref, raw, conv_ref, channel, taps, tokens):
    at = 0
    for part in raw:
        ext_ref[pl.ds(at, part.shape[0]), :] = part
        at += part.shape[0]
    summed = None
    for s in range(taps):
        part = conv_ref[channel, pl.ds(s, 1), :] * ext_ref[pl.ds(HALO - s, tokens), :]
        summed = part if summed is None else summed + part
    return jax.nn.silu(summed)


def unit_heads(values, heads, dim):
    parts = []
    for h in range(heads):
        v = values[:, h * dim : (h + 1) * dim]
        parts.append(v * lax.rsqrt(jnp.sum(v * v, axis=-1, keepdims=True) + 1.0))
    return jnp.concatenate(parts, axis=1)


def decay_of(running, running_t, unit):
    row, col = iotas(BLOCK)
    spread = running_t[:, unit : unit + 1] - running[unit : unit + 1, :]
    return jnp.where(row >= col, jnp.exp(jnp.minimum(spread, 0.0)), 0.0)


def take_pieces(refs, masks, chunks):
    return [[refs[m * chunks + c] for c in range(chunks)] for m in range(masks)]


def key_kernel(masks, chunks, heads, dim, taps, *refs):
    index = refs[0][0]
    decay_log, beta_bias, decay_bias = refs[1:4]
    refs = refs[4:]
    pieces = take_pieces(refs, masks, chunks)
    refs = refs[masks * chunks :]
    key_w, value_w, beta_w, decay_w, conv_ref = refs[:5]
    k_hbm, run_out, solved_hbm, prefix_hbm, slab_hbm, slab_low_out = refs[5:11]
    ext, k_out, solved_out, prefix_out, slab_out, sems = refs[11:]
    tokens = k_out.shape[0]
    leaving = [
        pltpu.make_async_copy(k_out, k_hbm, sems.at[0]),
        pltpu.make_async_copy(solved_out, solved_hbm, sems.at[1]),
        pltpu.make_async_copy(prefix_out, prefix_hbm, sems.at[2]),
        pltpu.make_async_copy(slab_out, slab_hbm, sems.at[3]),
    ]
    features = pieces[0][0].shape[1]
    blocks = tokens // BLOCK
    units = [(b, h) for b in range(blocks) for h in range(heads)]
    row, col = iotas(BLOCK)
    eye = jnp.where(row == col, 1.0, 0.0).astype(f32)

    beta_raw = project_rows(pieces, beta_w, index, features)
    decay_raw = project_rows(pieces, decay_w, index, features)
    beta_rows, log_rows = [], []
    for h in range(heads):
        beta_rows.append(jax.nn.sigmoid(beta_raw[h : h + 1] + beta_bias[h]))
        z = decay_raw[h : h + 1] + decay_bias[h]
        soft = jnp.maximum(z, 0.0) + jnp.log(1.0 + jnp.exp(-jnp.abs(z)))
        log_rows.append(-jnp.exp(jnp.full_like(z, decay_log[h])) * soft)

    def by_unit(rows):
        return jnp.concatenate(
            [rows[h][:, b * BLOCK : (b + 1) * BLOCK] for b, h in units], axis=0
        )

    running = lax.dot_general(
        by_unit(log_rows),
        jnp.where(row <= col, 1.0, 0.0).astype(f32),
        (((1,), (0,)), ((), ())),
        preferred_element_type=f32,
        precision=lax.Precision.HIGHEST,
    )
    run_out[...] = running
    running_t = jnp.transpose(running)
    beta_t = jnp.transpose(by_unit(beta_rows))
    keys = unit_heads(
        conv_rows(ext, project(pieces, key_w, index, features), conv_ref, 1, taps, tokens),
        heads,
        dim,
    )
    k_out[...] = keys
    leaving[0].start()
    values = conv_rows(
        ext, project(pieces, value_w, index, features), conv_ref, 2, taps, tokens
    )
    k_of = {}
    lower = {}
    inverse = {}
    for b, h in units:
        k = keys[b * BLOCK : (b + 1) * BLOCK, h * dim : (h + 1) * dim]
        k_of[b, h] = k
        pair = split(k)
        unit = b * heads + h
        gram = mm_nt(pair, pair)
        system = jnp.where(
            row > col,
            beta_t[:, unit : unit + 1] * decay_of(running, running_t, unit) * gram,
            0.0,
        )
        lower[b, h] = system
        link = (row // 2 == col // 2) & (row > col)
        inverse[b, h] = eye - jnp.where(link, system, 0.0)
    width = 2
    while width < BLOCK:
        link = (row // (2 * width) == col // (2 * width)) & (row // width > col // width)
        middle = {}
        pairs = {}
        for u in units:
            pairs[u] = split(inverse[u])
            middle[u] = mm_square(split(jnp.where(link, lower[u], 0.0)), pairs[u])
        for u in units:
            inverse[u] = inverse[u] - mm_square(pairs[u], split(middle[u]))
        width *= 2
    maps = {}
    solved_pair = {}
    for b, h in units:
        k = k_of[b, h]
        unit = b * heads + h
        bcol = beta_t[:, unit : unit + 1]
        rcol = running_t[:, unit : unit + 1]
        v = values[b * BLOCK : (b + 1) * BLOCK, h * dim : (h + 1) * dim]
        right = jnp.concatenate([(bcol * jnp.exp(rcol)) * k, bcol * v], axis=1)
        solved = mm_wide(split(inverse[b, h]), split(right))
        solved_out[b * heads + h] = solved
        solved_pair[b, h] = split(solved)
    leaving[1].start()
    for b, h in units:
        rcol = running_t[:, b * heads + h : b * heads + h + 1]
        last = rcol[BLOCK - 1 : BLOCK, :]
        weighted = jnp.transpose(jnp.exp(last - rcol) * k_of[b, h])
        moved = mm_wide(split(weighted), solved_pair[b, h])
        transit = jnp.exp(last) * eye - moved[:, :dim]
        maps[b, h] = jnp.concatenate([transit, moved[:, dim:]], axis=1)

    slabs = []
    for h in range(heads):
        spans = {(b, 1): maps[b, h] for b in range(blocks)}

        def span(start, count, h=h, spans=spans):
            if (start, count) not in spans:
                half = 1
                while half * 2 < count:
                    half *= 2
                spans[start, count] = compose(
                    span(start + half, count - half), span(start, half), dim
                )
            return spans[start, count]

        for b in range(1, blocks):
            prefix_out[h * (blocks - 1) + b - 1] = span(0, b)
        slabs.append(span)
    leaving[2].start()
    for h, span in enumerate(slabs):
        slab = span(0, blocks)
        slab_out[h] = slab
        slab_low_out[h] = slab.astype(bf16)
    leaving[3].start()
    for copy in leaving:
        copy.wait()


def query_kernel(masks, chunks, heads, dim, taps, *refs):
    index = refs[0][0]
    refs = refs[1:]
    pieces = take_pieces(refs, masks, chunks)
    query_w, gate_w, conv_ref, gain_ref = refs[masks * chunks : masks * chunks + 4]
    q_out, gate_out, ext = refs[masks * chunks + 4 :]
    tokens = q_out.shape[0]
    features = pieces[0][0].shape[1]
    raw = project(pieces, query_w, index, features)
    q_out[...] = unit_heads(conv_rows(ext, raw, conv_ref, 0, taps, tokens), heads, dim)
    gain = jnp.concatenate([gain_ref[...]] * heads, axis=1)
    at = 0
    for chunk, part in enumerate(project(pieces, gate_w, index, features)):
        part = part[HALO:] if chunk == 0 else part
        gate_out[pl.ds(at, part.shape[0]), :] = jax.nn.silu(part) * gain
        at += part.shape[0]


def read_kernel(heads, dim, q_ref, k_ref, run_ref, solved_ref, prefix_ref, a_out, r_out):
    tokens = q_ref.shape[0]
    blocks = tokens // BLOCK
    units = [(b, h) for b in range(blocks) for h in range(heads)]
    running = run_ref[...]
    running_t = jnp.transpose(running)
    mixing = {}
    for b, h in units:
        q = split(q_ref[pl.ds(b * BLOCK, BLOCK), pl.ds(h * dim, dim)])
        k = split(k_ref[pl.ds(b * BLOCK, BLOCK), pl.ds(h * dim, dim)])
        mixing[b, h] = decay_of(running, running_t, b * heads + h) * mm_nt(q, k)
    for b, h in units:
        rows, cols = pl.ds(b * BLOCK, BLOCK), pl.ds(h * dim, dim)
        out = mm_wide(split(mixing[b, h]), split(solved_ref[b * heads + h]))
        growth = jnp.exp(running_t[:, b * heads + h : b * heads + h + 1])
        reader = growth * q_ref[rows, cols] - out[:, :dim]
        local = out[:, dim:]
        if b > 0:
            moved = mm_wide(split(reader), split(prefix_ref[h * (blocks - 1) + b - 1]))
            reader = moved[:, :dim]
            local = local + moved[:, dim:]
        a_out[rows, cols] = local
        r_out[rows, cols] = reader


def compose(later, earlier, dim):
    out = mm_wide(split(later[:, :dim]), split(earlier))
    return jnp.concatenate([out[:, :dim], out[:, dim:] + later[:, dim:]], axis=1)


def own_kernel(in_ref, out_ref):
    out_ref[...] = in_ref[...]


def step_kernel(heads, dim, first, distance, pos_ref, got_ref, *refs):
    if first:
        own_ref, before_out, own_out, low_out = refs
    else:
        before_ref, own_ref, before_out, own_out, low_out = refs
    partner_earlier = (pos_ref[0] & distance) != 0
    row = lax.broadcasted_iota(jnp.int32, (dim, 2 * dim), 0)
    col = lax.broadcasted_iota(jnp.int32, (dim, 2 * dim), 1)
    unchanged = jnp.where(row == col, 1.0, 0.0).astype(f32)
    for h in range(heads):
        got = got_ref[h].astype(f32)
        mine = own_ref[h]
        own = compose(
            jnp.where(partner_earlier, mine, got), jnp.where(partner_earlier, got, mine), dim
        )
        own_out[h] = own
        low_out[h] = own[:, dim - low_out.shape[2] + dim :].astype(bf16)
        if first:
            before_out[h] = jnp.where(partner_earlier, got, unchanged)
        else:
            before = before_ref[h]
            before_out[h] = jnp.where(partner_earlier, compose(before, got, dim), before)


def hidden_kernel(heads, dim, distance, pos_ref, a_ref, r_ref, gate_ref, before_ref, got_ref, *outs):
    partner_earlier = (pos_ref[0] & distance) != 0
    rows = a_ref.shape[0] // len(outs)
    for h in range(heads):
        cols = pl.ds(h * dim, dim)
        before = before_ref[h]
        got = jnp.where(partner_earlier, got_ref[h].astype(f32), 0.0).astype(bf16)
        hi, lo = split(before[:, :dim])
        state = before[:, dim:] + dot(
            jnp.concatenate([hi, lo], axis=1), jnp.concatenate([got, got], axis=0)
        )
        out = a_ref[:, cols] + mm_square(split(r_ref[:, cols]), split(state))
        scaled = out * lax.rsqrt(jnp.mean(out * out, axis=-1, keepdims=True) + norm_floor)
        result = (scaled * gate_ref[:, cols]).astype(bf16)
        for c, out_ref in enumerate(outs):
            out_ref[:, cols] = result[c * rows : (c + 1) * rows]


def output_kernel(count, *refs):
    out_ref = refs[-1]
    total = None
    for m in range(count):
        part = dot(refs[m][...], refs[count + m][...])
        total = part if total is None else total + part
    out_ref[...] = total.astype(out_ref.dtype)


def xor_permute(value, mask):
    count = lax.axis_size("head")
    return lax.ppermute(value, "head", [(i, i ^ mask) for i in range(count)])


def gather_chunks(parts, masks):
    order = []
    bit = masks // 2
    while bit >= 1:
        order.append(bit)
        bit //= 2
    pieces = {0: list(parts)}
    for bit in order:
        for mask in sorted(pieces):
            got = list(pieces[mask])
            for c in reversed(range(len(got))):
                got[c] = xor_permute(got[c], bit)
            pieces[mask | bit] = got
    return [pieces[m] for m in range(masks)]


def vmem_call(kernel, out_shape, operands, scalars=0, scratch=(), limit=16, hbm=()):
    specs = [
        pl.BlockSpec(memory_space=pltpu.SMEM if i < scalars else pltpu.VMEM)
        for i in range(len(operands))
    ]
    outs = pl.BlockSpec(memory_space=pltpu.VMEM)
    if isinstance(out_shape, tuple):
        outs = tuple(
            pl.BlockSpec(memory_space=pltpu.HBM if i in hbm else pltpu.VMEM)
            for i in range(len(out_shape))
        )
        out_shape = tuple(
            pltpu.HBM(o.shape, o.dtype) if i in hbm else o for i, o in enumerate(out_shape)
        )
    return pl.pallas_call(
        kernel,
        out_shape=out_shape,
        in_specs=specs,
        out_specs=outs,
        scratch_shapes=list(scratch),
        compiler_params=pltpu.CompilerParams(vmem_limit_bytes=limit * 2**20),
    )(*operands)


def on_device(
    layer_in,
    query_weight,
    key_weight,
    value_weight,
    gate_weight,
    beta_weight,
    decay_weight,
    conv_weight,
    decay_log,
    beta_bias,
    decay_bias,
    norm_gain,
    out_weight,
):
    tokens, _ = layer_in.shape
    heads = beta_weight.shape[1]
    channels = query_weight.shape[1]
    dim = channels // heads
    taps = conv_weight.shape[0]
    masks = lax.axis_size("head")
    slabs = lax.axis_size("seq")
    blocks = tokens // BLOCK
    head = lax.axis_index("head")
    head_at = head.reshape(1).astype(jnp.int32)
    pos_at = lax.axis_index("seq").reshape(1).astype(jnp.int32)

    def shifted(value, distance):
        pairs = [(s, s + distance) for s in range(slabs - distance)]
        return lax.ppermute(value, "seq", pairs)

    chunks = 2
    step = tokens // chunks
    halo = shifted(layer_in[tokens - HALO :], 1)
    first = jnp.concatenate([halo, layer_in[:step]], axis=0)
    x_pieces = gather_chunks([first, layer_in[step:]], masks)
    x_flat = [c for piece in x_pieces for c in piece]
    conv = conv_weight.transpose(1, 0, 2)
    gain = norm_gain[None]

    shape = jax.ShapeDtypeStruct
    ext = pltpu.VMEM((tokens + HALO, channels), f32)
    maps = (heads, dim, 2 * dim)
    rows = (tokens, channels)
    keys, running, solved, prefix, slab, slab_low = vmem_call(
        functools.partial(key_kernel, masks, chunks, heads, dim, taps),
        (
            shape(rows, f32),
            shape((blocks * heads, BLOCK), f32),
            shape((blocks * heads, BLOCK, 2 * dim), f32),
            shape(((blocks - 1) * heads, dim, 2 * dim), f32),
            shape(maps, f32),
            shape(maps, bf16),
        ),
        [head_at, decay_log, beta_bias, decay_bias, *x_flat]
        + [key_weight, value_weight, beta_weight.T, decay_weight.T, conv],
        scalars=4,
        scratch=(
            ext,
            pltpu.VMEM(rows, f32),
            pltpu.VMEM((blocks * heads, BLOCK, 2 * dim), f32),
            pltpu.VMEM(((blocks - 1) * heads, dim, 2 * dim), f32),
            pltpu.VMEM(maps, f32),
            pltpu.SemaphoreType.DMA((4,)),
        ),
        limit=24,
        hbm=(0, 2, 3, 4),
    )

    width = out_weight.shape[1] // masks
    sends = [
        lax.dynamic_slice(out_weight, (0, (head ^ m) * width), (channels, width))
        for m in range(masks)
    ]
    columns = [sends[0]]
    held, _ = lax.optimization_barrier((sends, x_pieces[masks // 2]))
    for m in range(1, masks):
        columns.append(xor_permute(held[m], m))

    x_late, _ = lax.optimization_barrier((x_flat, slab_low))
    queries, gates = vmem_call(
        functools.partial(query_kernel, masks, chunks, heads, dim, taps),
        (shape(rows, f32), shape(rows, f32)),
        [head_at, *x_late, query_weight, gate_weight, conv, gain],
        scalars=1,
        scratch=(ext,),
        limit=16,
    )

    def exchanged(value, distance):
        pairs = [(s, s ^ distance) for s in range(slabs)]
        return lax.ppermute(value, "seq", pairs)

    before = None
    distance = 1
    while 2 * distance < slabs:
        got = exchanged(slab_low, distance)
        if before is None:
            slab = vmem_call(own_kernel, shape(maps, f32), [slab], limit=8)
        operands = [pos_at, got] + ([] if before is None else [before]) + [slab]
        sent = dim if 4 * distance >= slabs else 2 * dim
        before, slab, slab_low = vmem_call(
            functools.partial(step_kernel, heads, dim, before is None, distance),
            (shape(maps, f32), shape(maps, f32), shape((heads, dim, sent), bf16)),
            operands,
            scalars=1,
            limit=8,
        )
        distance *= 2
    got = exchanged(slab_low, distance)
    local, reader = vmem_call(
        functools.partial(read_kernel, heads, dim),
        (shape(rows, f32), shape(rows, f32)),
        [queries, keys, running, solved, prefix],
        limit=16,
    )
    half = (tokens // 2, channels)
    hidden = vmem_call(
        functools.partial(hidden_kernel, heads, dim, distance),
        (shape(half, bf16), shape(half, bf16)),
        [pos_at, local, reader, gates, before, got],
        scalars=1,
        limit=8,
    )
    pieces = gather_chunks(hidden, masks)
    result = None
    whole = pl.BlockSpec(memory_space=pltpu.VMEM)
    for c in reversed(range(2)):
        operands = [p[c] for p in pieces] + columns
        specs = [whole] * len(operands)
        aliases = {}
        if result is not None:
            aliases = {len(operands): 0}
            operands.append(result)
            specs.append(pl.BlockSpec(memory_space=pl.ANY))
        result = pl.pallas_call(
            functools.partial(output_kernel, masks),
            grid=(1,),
            out_shape=shape((tokens, width), bf16),
            in_specs=specs,
            out_specs=pl.BlockSpec((tokens // 2, width), lambda i, c=c: (c, 0)),
            input_output_aliases=aliases,
            compiler_params=pltpu.CompilerParams(vmem_limit_bytes=8 * 2**20),
        )(*operands)
    return result


def solution(mesh):
    return jax.shard_map(
        on_device,
        mesh=mesh,
        in_specs=(
            P("seq", "head"),
            P(None, "head"),
            P(None, "head"),
            P(None, "head"),
            P(None, "head"),
            P(None, "head"),
            P(None, "head"),
            P(None, None, "head"),
            P("head"),
            P("head"),
            P("head"),
            P(),
            P("head", None),
        ),
        out_specs=P("seq", "head"),
        check_vma=False,
    )
```
